768 devices in a mesh: dp: 12 (over z), mp: 64 (over x, y, core).
Axes of the slice: x: 4, y: 8, z: 12, core: 2. Of those that a mesh axis runs over, the one named last changes fastest.
Arguments:
- grad_parts: bfloat16 [12, 64, 2, 2304, 128], P('dp', 'mp'), may hold values from -45 to 45
- master: float32 [64, 2, 2304, 128], P('mp', None, 'dp'), may hold values from -15 to 15
- momenta: float32 [3, 64, 2, 2304, 128], P(None, 'mp', None, 'dp'), may hold values from -45 to 45
- second: float32 [3, 64, 2, 2304, 128], P(None, 'mp', None, 'dp'), may hold values from 0.00025 to 330
- step_count: int32 [1], replicated, may hold values from 1 to 99999
- mlp_first: float32 [8, 4], replicated, may hold values from -2 to 2
- mlp_bias: float32 [4], replicated, may hold values from -3 to 3
- mlp_second: float32 [4, 2], replicated, may hold values from -3 to 3
- tensor_weight: float32 [10], replicated, may hold values from -2 to 2
Outputs:
- new_params: bfloat16 [64, 2, 2304, 128], P('mp')
- new_master: float32 [64, 2, 2304, 128], P('mp', None, 'dp')
- new_momenta: float32 [3, 64, 2, 2304, 128], P(None, 'mp', None, 'dp')
- new_second: float32 [3, 64, 2, 2304, 128], P(None, 'mp', None, 'dp')
- update: float32 [64, 2, 2304, 128], P('mp', None, 'dp')
The draws below stay inside these ranges and needn't reach their ends.
All inputs are finite; a program needn't handle non-finite values.
Results may differ from the reference program's by a relative error of at most 0.019.
Values may be sent and summed in bfloat16 or wider, within the bound.
No kernel may reach another device: no remote copies, remote signals or barrier semaphores. Data moves between devices by JAX's collectives and lax.ppermute only.
A program may use at most 32 MiB of HBM per device.

```python
import jax
import jax.numpy as jnp
from jax import lax

D = 4608
HQ = 4096
LANES = 128
FEATS = 8
HIDDEN_UNITS = 4
NT = 2
ROWS = 2304
OWN = 192
N_DP = 12
N_MP = 64


def texture(key):
    key_rows = jax.random.fold_in(key, 1)
    key_lanes = jax.random.fold_in(key, 2)
    key_blocks = jax.random.fold_in(key, 3)
    position = jnp.arange(N_MP, dtype=jnp.float32) / max(N_MP - 1, 1)
    rising = jnp.exp(jnp.log(3.0) * position)[:, None, None, None]
    owner = jnp.arange(N_DP, dtype=jnp.float32) / max(N_DP - 1, 1)
    owner_rise = jnp.exp(jnp.log(3.0) * (owner - 1.0))[None, None, :, None, None]
    owner_random = jnp.exp(jax.random.uniform(key_blocks, (N_MP, NT, N_DP, 1, 1), minval=-jnp.log(3.0), maxval=0.0))
    row_part = jnp.exp(jax.random.uniform(key_rows, (N_MP, NT, N_DP, OWN, 1), minval=0.0, maxval=jnp.log(5.0)))
    row_part = (row_part * owner_rise * owner_random).reshape(N_MP, NT, ROWS, 1)
    lane_part = jnp.exp(jax.random.uniform(key_lanes, (1, NT, 1, LANES), minval=0.0, maxval=jnp.log(2.0)))
    return rising * row_part * lane_part


def draw_grad_parts(key, part):
    scales = texture(jax.random.fold_in(key, 11))
    ratio = jnp.exp(jnp.log(3.0) * jnp.arange(N_DP, dtype=jnp.float32) / max(N_DP - 1, 1))[:, None, None, None, None]
    key_noise = jax.random.fold_in(key, 12)
    noise = jax.random.truncated_normal(key_noise, -5.0, 5.0, (N_DP, N_MP, NT, ROWS, LANES))
    values = 0.1 * ratio * scales * noise
    return values.astype(jnp.bfloat16)


def draw_master(key, part):
    scales = texture(jax.random.fold_in(key, 21))
    key_noise = jax.random.fold_in(key, 22)
    noise = jax.random.truncated_normal(key_noise, -5.0, 5.0, (N_MP, NT, ROWS, LANES))
    return 0.1 * scales * noise


def draw_momenta(key, part):
    scales = texture(jax.random.fold_in(key, 31))
    key_noise = jax.random.fold_in(key, 32)
    noise = jax.random.truncated_normal(key_noise, -5.0, 5.0, (3, N_MP, NT, ROWS, LANES))
    return 0.3 * scales[None] * noise


def draw_second(key, part):
    scales = texture(jax.random.fold_in(key, 41))
    key_noise = jax.random.fold_in(key, 42)
    factor = jnp.exp(jax.random.uniform(key_noise, (3, N_MP, NT, ROWS, LANES), minval=jnp.log(0.25), maxval=jnp.log(4.0)))
    base = 0.3 * scales
    return (base * base)[None] * factor


def centred(stream_key, extent, deviation, most, kind=jnp.bfloat16):
    result = jax.random.normal(stream_key, extent, jnp.float32) * deviation
    return jnp.minimum(jnp.maximum(result, -most), most).astype(kind)


def setup_inputs(seed: int = 0) -> dict:
    key_list = jax.random.split(jax.random.key(seed), 10)
    return {
        "grad_parts": draw_grad_parts(jax.random.fold_in(key_list[9], 71), 0),
        "master": draw_master(jax.random.fold_in(key_list[9], 71), 0),
        "momenta": draw_momenta(jax.random.fold_in(key_list[9], 71), 0),
        "second": draw_second(jax.random.fold_in(key_list[9], 71), 0),
        "step_count": jax.random.randint(key_list[4], (1,), 1, 100000).astype(jnp.int32),
        "mlp_first": centred(key_list[5], (FEATS, HIDDEN_UNITS), FEATS ** -0.5, 2.0, jnp.float32),
        "mlp_bias": centred(key_list[6], (HIDDEN_UNITS,), 0.5, 3.0, jnp.float32),
        "mlp_second": centred(key_list[7], (HIDDEN_UNITS, 2), HIDDEN_UNITS ** -0.5, 3.0, jnp.float32),
        "tensor_weight": centred(key_list[8], (FEATS + 2,), 0.3, 2.0, jnp.float32),
    }


RATES = (0.9, 0.99, 0.999)

def features_of(master, gradient, moments, squares):
    listing = [master, gradient, moments[0], moments[1], moments[2]]
    for slot_id in range(3):
        listing.append(moments[slot_id] / jnp.sqrt(squares[slot_id]))
    return listing

def perceptron(normed, boost, mlp_first, mlp_bias, mlp_second):
    direction = jnp.zeros_like(normed[0])
    magnitude = jnp.zeros_like(normed[0])
    for unit_id in range(mlp_first.shape[1]):
        active = mlp_first[0, unit_id] * normed[0]
        for feat_id in range(1, len(normed)):
            active = active + mlp_first[feat_id, unit_id] * normed[feat_id]
        active = jax.nn.relu(active + mlp_bias[unit_id])
        direction = direction + mlp_second[unit_id, 0] * active
        magnitude = magnitude + mlp_second[unit_id, 1] * active
    return direction * jnp.exp(0.5 * jnp.tanh(magnitude)) * boost

def tensor_boost(norms, step_count, tensor_weight):
    count = tensor_weight.shape[0] - 2
    step_value = step_count[0].astype(jnp.float32)
    first_phase = jnp.log1p(step_value) / 11.5
    second_phase = step_value / 100000.0
    logits = lax.optimization_barrier(jnp.sum(tensor_weight[:count, None] * jnp.log(norms), axis=0))
    logits = logits + tensor_weight[count] * first_phase + tensor_weight[count + 1] * second_phase
    return jnp.exp(jnp.tanh(logits))

def reference(grad_parts, master, momenta, second, step_count, mlp_first, mlp_bias, mlp_second, tensor_weight):
    gradient = lax.optimization_barrier(jnp.sum(grad_parts, axis=0, dtype=jnp.float32))
    new_momenta = jnp.stack([rate * momenta[i] + (1.0 - rate) * gradient for i, rate in enumerate(RATES)])
    new_second = jnp.stack([rate * second[i] + (1.0 - rate) * gradient * gradient for i, rate in enumerate(RATES)])
    listing = features_of(master, gradient, new_momenta, new_second)
    totals = jnp.stack([lax.optimization_barrier(jnp.sum(feature * feature, axis=(0, 2, 3))) for feature in listing])
    norms = jnp.sqrt(totals / float(D * HQ) + 1e-06)
    boost = tensor_boost(norms, step_count, tensor_weight)[None, :, None, None]
    normed = [listing[i] / norms[i][None, :, None, None] for i in range(len(listing))]
    update = perceptron(normed, boost, mlp_first, mlp_bias, mlp_second)
    new_master = master - 0.05 * update
    new_params = new_master.astype(jnp.bfloat16)
    return (new_params, new_master, new_momenta, new_second, update)
```

```python
import jax
import jax.numpy as jnp
from jax import lax
from jax.experimental import pallas as pl
from jax.experimental.pallas import tpu as pltpu
from jax.sharding import Mesh
from jax.sharding import PartitionSpec as P

D = 4608
HQ = 4096
DP = ("hi", "lo")
MP = ("mp_0", "mp_1", "mp_2")
RATES = (0.9, 0.99, 0.999)
FEATS = 8
HIDDEN = 4
NT = 2
LANES = 128
STEP = 32
LATE = 48

VMEM = pl.BlockSpec(memory_space=pltpu.VMEM)
SMEM = pl.BlockSpec(memory_space=pltpu.SMEM)


def ratio_of(moment, square):
    return moment * lax.rsqrt(square)


def reduced_gradient(parts):
    hi_count, lo_count = lax.axis_size("hi"), lax.axis_size("lo")
    count = hi_count * lo_count
    lo = lax.axis_index("lo")
    nt, rows, lanes = parts.shape
    blocks = parts.reshape(nt, hi_count, lo_count, rows // count, lanes)

    def of_class(shift):
        return lax.dynamic_index_in_dim(blocks, (lo + shift) % lo_count, 2, keepdims=False)

    from_below = lax.ppermute(of_class(1), DP, [(i, (i + 1) % count) for i in range(count)])
    from_above = lax.ppermute(of_class(lo_count - 1), DP, [(i, (i - 1) % count) for i in range(count)])
    partial = of_class(0).astype(jnp.float32) + from_below.astype(jnp.float32)
    partial = (partial + from_above.astype(jnp.float32)).astype(jnp.bfloat16)
    return lax.all_to_all(jnp.moveaxis(partial, 1, 0), "hi", 0, 0, tiled=True)


def moments_kernel(got, master, momenta, second, grad_out, momenta_out, second_out, sums_out, table):
    own = master.shape[0] // NT
    table[...] = jnp.zeros_like(table)
    for t in range(NT):

        def body(i, sums):
            rows = pl.ds(pl.multiple_of(t * own + i * STEP, STEP), STEP)
            grad = got[0, rows, :].astype(jnp.float32)
            for k in range(1, got.shape[0]):
                grad = grad + got[k, rows, :].astype(jnp.float32)
            grad_out[rows, :] = grad
            square = grad * grad
            listing = [master[rows, :], grad]
            ratios = []
            for k, rate in enumerate(RATES):
                moment = rate * momenta[k, rows, :] + (1.0 - rate) * grad
                spread = rate * second[k, rows, :] + (1.0 - rate) * square
                momenta_out[k, rows, :] = moment
                second_out[k, rows, :] = spread
                listing.append(moment)
                ratios.append(ratio_of(moment, spread))
            listing = listing + ratios
            return tuple(
                s + jnp.sum((x * x).reshape(STEP // 8, 8, LANES), axis=0)
                for s, x in zip(sums, listing)
            )

        zeros = tuple(jnp.zeros((8, LANES), jnp.float32) for _ in range(FEATS))
        sums = lax.fori_loop(0, own // STEP, body, zeros)
        for f in range(FEATS):
            k = t * FEATS + f
            table[k : k + 1, :] = jnp.sum(sums[f], axis=0, keepdims=True)
    sums_out[...] = lax.dot_general(
        jnp.ones(sums_out.shape, jnp.float32),
        table[...],
        (((1,), (1,)), ((), ())),
        precision=lax.Precision.HIGHEST,
        preferred_element_type=jnp.float32,
    )


def spread_kernel(got, out):
    out[...] = jnp.broadcast_to(jnp.sum(got[...], axis=0, keepdims=True), out.shape)


def update_kernel(
    totals, lane_weight, phase, first, bias, last, master, grad, momenta, second,
    update_out, master_out, params_out, late_out, scaled,
):
    own = master.shape[0] // NT
    early = params_out.shape[0]
    total = jnp.sum(totals[...], axis=0, keepdims=True)
    norms = jnp.sqrt(total / float(D * HQ) + 1e-06)
    inverse = 1.0 / norms
    logs = lane_weight[...] * jnp.log(norms)
    lane = lax.broadcasted_iota(jnp.int32, logs.shape, 1)
    for t in range(NT):
        mine = jnp.where(lane // FEATS == t, logs, 0.0)
        logit = jnp.sum(mine, axis=1, keepdims=True) + phase[0]
        boost = jnp.broadcast_to(jnp.exp(jnp.tanh(logit)), (8, LANES))
        for f in range(FEATS):
            k = t * FEATS + f
            scale = jnp.broadcast_to(inverse[:, k : k + 1], (8, LANES))
            for j in range(HIDDEN):
                scaled[f * HIDDEN + j] = first[f, j] * scale

        def rows_of(x):
            return jnp.broadcast_to(x[None], (STEP // 8, 8, LANES)).reshape(STEP, LANES)

        boost = rows_of(boost)

        def one(start):
            rows = pl.ds(start, STEP)
            old = master[rows, :]
            moments = [momenta[k, rows, :] for k in range(len(RATES))]
            listing = [old, grad[rows, :], *moments]
            listing += [ratio_of(moments[k], second[k, rows, :]) for k in range(len(RATES))]
            direction = jnp.zeros((STEP, LANES), jnp.float32)
            magnitude = jnp.zeros((STEP, LANES), jnp.float32)
            for j in range(HIDDEN):
                active = bias[j] + listing[0] * rows_of(scaled[j])
                for f in range(1, FEATS):
                    active = active + listing[f] * rows_of(scaled[f * HIDDEN + j])
                active = jnp.maximum(active, 0.0)
                direction = direction + last[j, 0] * active
                magnitude = magnitude + last[j, 1] * active
            step = direction * jnp.exp(0.5 * jnp.tanh(magnitude)) * boost
            new = old - 0.05 * step
            update_out[rows, :] = step
            master_out[rows, :] = new
            return new.astype(jnp.bfloat16)

        def body(i, carry):
            start = pl.multiple_of(t * own + i * STEP, STEP)
            params_out[pl.ds(start, STEP), :] = one(start)
            return carry

        last_early = min(early, (t + 1) * own)
        lax.fori_loop(0, (last_early - t * own) // STEP, body, 0)
        for start in range(last_early - (last_early - t * own) % STEP, (t + 1) * own, STEP):
            both = one(start)
            if start < early:
                params_out[start:early, :] = both[: early - start]
                both = both[early - start :]
            place = max(start, early) - early
            for copy in range(late_out.shape[0]):
                late_out[copy, place : place + both.shape[0], :] = both


def local(
    grad_parts, master, momenta, second, step_count, mlp_first, mlp_bias, mlp_second, tensor_weight
):
    dp_count = lax.axis_size("hi") * lax.axis_size("lo")
    mp_count = lax.axis_size("mp_0") * lax.axis_size("mp_1") * lax.axis_size("mp_2")
    _, nt, own, lanes = master.shape
    rows = nt * own
    early = rows - LATE
    f32 = jnp.float32
    state = jax.ShapeDtypeStruct((rows, lanes), f32)
    triple = jax.ShapeDtypeStruct((3, rows, lanes), f32)

    got = reduced_gradient(grad_parts[0, 0])
    old_master = master.reshape(rows, lanes)
    grad, new_momenta, new_second, sums = pl.pallas_call(
        moments_kernel,
        out_shape=(state, triple, triple, jax.ShapeDtypeStruct((mp_count, lanes), f32)),
        in_specs=[VMEM] * 4,
        out_specs=(VMEM,) * 4,
        scratch_shapes=[pltpu.VMEM((LANES, LANES), f32)],
        name="moments",
    )(
        got.reshape(-1, rows, lanes),
        old_master,
        momenta.reshape(3, rows, lanes),
        second.reshape(3, rows, lanes),
    )
    sums = lax.all_to_all(sums, MP, 0, 0, tiled=True)
    sums = pl.pallas_call(
        spread_kernel,
        out_shape=jax.ShapeDtypeStruct((dp_count, lanes), f32),
        in_specs=[VMEM],
        out_specs=VMEM,
        name="spread",
    )(sums)
    sums = lax.all_to_all(sums, DP, 0, 0, tiled=True)

    step_value = step_count[0].astype(f32)
    phase = tensor_weight[FEATS] * (jnp.log1p(step_value) / 11.5)
    phase = phase + tensor_weight[FEATS + 1] * (step_value / 100000.0)
    lane_weight = jnp.pad(jnp.tile(tensor_weight[:FEATS], nt), (0, lanes - nt * FEATS))[None]
    update, new_master, params, late = pl.pallas_call(
        update_kernel,
        out_shape=(
            state,
            state,
            jax.ShapeDtypeStruct((early, lanes), jnp.bfloat16),
            jax.ShapeDtypeStruct((dp_count, LATE, lanes), jnp.bfloat16),
        ),
        in_specs=[VMEM, VMEM, SMEM, SMEM, SMEM, SMEM, VMEM, VMEM, VMEM, VMEM],
        out_specs=(VMEM,) * 4,
        scratch_shapes=[pltpu.VMEM((FEATS * HIDDEN, 8, LANES), f32)],
        name="update",
    )(
        sums, lane_weight, phase[None], mlp_first, mlp_bias, mlp_second,
        old_master, grad, new_momenta, new_second,
    )
    late = lax.all_to_all(late, DP, 0, 0, tiled=True)
    params = lax.all_gather(params, DP, axis=0, tiled=False)
    second_part = jnp.concatenate([params[:, own:], late], axis=1)
    new_params = jnp.stack([params[:, :own], second_part]).reshape(1, nt, dp_count * own, lanes)
    shape = master.shape
    return (
        new_params,
        new_master.reshape(shape),
        new_momenta.reshape(3, *shape),
        new_second.reshape(3, *shape),
        update.reshape(shape),
    )


def solution(mesh):
    torus = Mesh(mesh.devices.reshape(mesh.shape["dp"] // 3, 3, 4, 8, 2), (*DP, *MP))
    return jax.shard_map(
        local,
        mesh=torus,
        in_specs=(
            P(DP, MP, None, None, None),
            P(MP, None, DP, None),
            P(None, MP, None, DP, None),
            P(None, MP, None, DP, None),
            P(),
            P(),
            P(),
            P(),
            P(),
        ),
        out_specs=(
            P(MP, None, None, None),
            P(MP, None, DP, None),
            P(None, MP, None, DP, None),
            P(None, MP, None, DP, None),
            P(MP, None, DP, None),
        ),
        check_vma=False,
    )
```

```python
import jax
import jax.numpy as jnp
from jax import lax
from jax.experimental import pallas as pl
from jax.experimental.pallas import tpu as pltpu
from jax.sharding import Mesh
from jax.sharding import PartitionSpec as P

D = 4608
HQ = 4096
DP = ("hi", "lo")
MP = ("mp_0", "mp_1", "mp_2")
RATES = (0.9, 0.99, 0.999)
FEATS = 8
HIDDEN = 4
NT = 2
LANES = 128
STEP = 32
TAIL = 16
GRADES = 8

VMEM = pl.BlockSpec(memory_space=pltpu.VMEM)
SMEM = pl.BlockSpec(memory_space=pltpu.SMEM)
PARAMS = pltpu.CompilerParams(vmem_limit_bytes=6 << 20)


def reduced_gradient(parts):
    hi_count, lo_count = lax.axis_size("hi"), lax.axis_size("lo")
    count = hi_count * lo_count
    lo = lax.axis_index("lo")
    nt, rows, lanes = parts.shape
    blocks = parts.reshape(nt, hi_count, lo_count, rows // count, lanes)

    def of_class(shift):
        return lax.dynamic_index_in_dim(blocks, (lo + shift) % lo_count, 2, keepdims=False)

    from_below = lax.ppermute(of_class(1), DP, [(i, (i + 1) % count) for i in range(count)])
    from_above = lax.ppermute(of_class(lo_count - 1), DP, [(i, (i - 1) % count) for i in range(count)])
    partial = of_class(0).astype(jnp.float32) + from_below.astype(jnp.float32)
    partial = (partial + from_above.astype(jnp.float32)).astype(jnp.bfloat16)
    return lax.all_to_all(jnp.moveaxis(partial, 1, 0), "hi", 0, 0, tiled=True)


def moments_kernel(got, master, momenta, second, features_out, sums_out, table):
    own = master.shape[0] // NT
    table[...] = jnp.zeros_like(table)
    for t in range(NT):

        def body(i, sums):
            rows = pl.ds(pl.multiple_of(t * own + i * STEP, STEP), STEP)
            grad = got[0, rows, :].astype(jnp.float32)
            for k in range(1, got.shape[0]):
                grad = grad + got[k, rows, :].astype(jnp.float32)
            square = grad * grad
            moments, ratios = [], []
            for k, rate in enumerate(RATES):
                moment = rate * momenta[k, rows, :] + (1.0 - rate) * grad
                spread = rate * second[k, rows, :] + (1.0 - rate) * square
                moments.append(moment)
                ratios.append(moment * lax.rsqrt(spread))
            listing = [grad, *moments, *ratios]
            for k, x in enumerate(listing):
                features_out[k, rows, :] = x
            return tuple(
                s + jnp.sum((x * x).reshape(STEP // 8, 8, LANES), axis=0)
                for s, x in zip(sums, [master[rows, :], *listing])
            )

        zeros = tuple(jnp.zeros((8, LANES), jnp.float32) for _ in range(FEATS))
        sums = lax.fori_loop(0, own // STEP, body, zeros)
        for f in range(FEATS):
            k = t * FEATS + f
            table[k : k + 1, :] = jnp.sum(sums[f], axis=0, keepdims=True)
    sums_out[...] = lax.dot_general(
        jnp.ones(sums_out.shape, jnp.float32),
        table[...],
        (((1,), (1,)), ((), ())),
        precision=lax.Precision.HIGHEST,
        preferred_element_type=jnp.float32,
    )


def update_kernel(
    totals, lane_weight, phase, first, bias, last, master, features,
    update_out, master_out, params_out, scaled,
):
    rows = master.shape[0]
    own = rows // NT
    total = jnp.sum(totals[...], axis=0, keepdims=True)
    norms = jnp.sqrt(total / float(D * HQ) + 1e-06)
    inverse = 1.0 / norms
    logs = lane_weight[...] * jnp.log(norms)
    lane = lax.broadcasted_iota(jnp.int32, logs.shape, 1)

    def rows_of(x):
        return jnp.broadcast_to(x[None], (STEP // 8, 8, LANES)).reshape(STEP, LANES)

    largest = jnp.zeros((8, LANES), jnp.float32)
    for t in range(NT):
        mine = jnp.where(lane // FEATS == t, logs, 0.0)
        logit = jnp.sum(mine, axis=1, keepdims=True) + phase[0]
        boost = rows_of(jnp.broadcast_to(jnp.exp(jnp.tanh(logit)), (8, LANES)))
        for f in range(FEATS):
            k = t * FEATS + f
            scale = jnp.broadcast_to(inverse[:, k : k + 1], (8, LANES))
            for j in range(HIDDEN):
                scaled[f * HIDDEN + j] = first[f, j] * scale

        def body(i, largest):
            at = pl.ds(pl.multiple_of(t * own + i * STEP, STEP), STEP)
            old = master[at, :]
            listing = [old] + [features[k, at, :] for k in range(FEATS - 1)]
            direction = jnp.zeros((STEP, LANES), jnp.float32)
            magnitude = jnp.zeros((STEP, LANES), jnp.float32)
            for j in range(HIDDEN):
                active = bias[j] + listing[0] * rows_of(scaled[j])
                for f in range(1, FEATS):
                    active = active + listing[f] * rows_of(scaled[f * HIDDEN + j])
                active = jnp.maximum(active, 0.0)
                direction = direction + last[j, 0] * active
                magnitude = magnitude + last[j, 1] * active
            step = direction * jnp.exp(0.5 * jnp.tanh(magnitude)) * boost
            new = old - 0.05 * step
            update_out[at, :] = step
            master_out[at, :] = new
            return jnp.maximum(largest, jnp.max(jnp.abs(new).reshape(STEP // 8, 8, LANES), axis=0))

        largest = lax.fori_loop(0, own // STEP, body, largest)

    most = jnp.max(jnp.max(largest, axis=0, keepdims=True), axis=1, keepdims=True) * 0.125
    power = jnp.full((1, 1), 0.125, jnp.float32)
    grades = jnp.ones((1, LANES), jnp.float32)
    for k in range(GRADES):
        small = most < 8.0
        most = jnp.where(small, most * 4096.0, most)
        power = jnp.where(small, power * 4096.0, power)
        grades = jnp.where(jnp.logical_and(small, lane == k), 1.0 / 4096.0, grades)
    power = jnp.broadcast_to(power, (STEP, LANES))

    def write(i, carry):
        at = pl.ds(pl.multiple_of(i * STEP, STEP), STEP)
        rounded = master_out[at, :].astype(jnp.bfloat16).astype(jnp.float32)
        params_out[at, :] = (rounded * power).astype(params_out.dtype)
        return carry

    lax.fori_loop(0, rows // STEP, write, 0)
    params_out[rows:, :] = jnp.broadcast_to(grades, (TAIL, LANES)).astype(params_out.dtype)


def local(
    grad_parts, master, momenta, second, step_count, mlp_first, mlp_bias, mlp_second, tensor_weight
):
    dp_count = lax.axis_size("hi") * lax.axis_size("lo")
    mp_count = lax.axis_size("mp_0") * lax.axis_size("mp_1") * lax.axis_size("mp_2")
    _, nt, own, lanes = master.shape
    rows = nt * own
    f32, bf16 = jnp.float32, jnp.bfloat16
    state = jax.ShapeDtypeStruct((rows, lanes), f32)

    got = reduced_gradient(grad_parts[0, 0])
    old_master = master.reshape(rows, lanes)
    old_second = second.reshape(3, rows, lanes)
    features, sums = pl.pallas_call(
        moments_kernel,
        out_shape=(
            jax.ShapeDtypeStruct((FEATS - 1, rows, lanes), f32),
            jax.ShapeDtypeStruct((mp_count, lanes), f32),
        ),
        in_specs=[VMEM] * 4,
        out_specs=(VMEM,) * 2,
        scratch_shapes=[pltpu.VMEM((LANES, LANES), f32)],
        compiler_params=PARAMS,
        name="moments",
    )(got.reshape(-1, rows, lanes), old_master, momenta.reshape(3, rows, lanes), old_second)
    sums = lax.all_to_all(sums, MP, 0, 0, tiled=True)
    sums = jnp.broadcast_to(jnp.sum(sums, axis=0), (dp_count, lanes))
    sums = lax.all_to_all(sums, DP, 0, 0, tiled=True)

    new_momenta = features[1:4]
    square = features[0] * features[0]
    new_second = jnp.stack(
        [rate * old_second[k] + (1.0 - rate) * square for k, rate in enumerate(RATES)]
    )

    step_value = step_count[0].astype(f32)
    phase = tensor_weight[FEATS] * (jnp.log1p(step_value) / 11.5)
    phase = phase + tensor_weight[FEATS + 1] * (step_value / 100000.0)
    lane_weight = jnp.pad(jnp.tile(tensor_weight[:FEATS], nt), (0, lanes - nt * FEATS))[None]
    update, new_master, params = pl.pallas_call(
        update_kernel,
        out_shape=(state, state, jax.ShapeDtypeStruct((rows + TAIL, lanes), bf16)),
        in_specs=[VMEM, VMEM, SMEM, SMEM, SMEM, SMEM, VMEM, VMEM],
        out_specs=(VMEM,) * 3,
        scratch_shapes=[pltpu.VMEM((FEATS * HIDDEN, 8, LANES), f32)],
        compiler_params=PARAMS,
        name="update",
    )(sums, lane_weight, phase[None], mlp_first, mlp_bias, mlp_second, old_master, features)
    params = lax.all_gather(params.astype(jnp.float16), DP, axis=0, tiled=False)
    scale = 8.0 * jnp.prod(params[:, rows, :GRADES].astype(f32), axis=1)
    params = params[:, :rows].astype(f32) * scale[:, None, None]
    params = params.astype(bf16).reshape(dp_count, nt, own, lanes)
    new_params = jnp.moveaxis(params, 0, 1).reshape(1, nt, dp_count * own, lanes)
    shape = master.shape
    return (
        new_params,
        new_master.reshape(shape),
        new_momenta.reshape(3, *shape),
        new_second.reshape(3, *shape),
        update.reshape(shape),
    )


def solution(mesh):
    torus = Mesh(mesh.devices.reshape(mesh.shape["dp"] // 3, 3, 4, 8, 2), (*DP, *MP))
    return jax.shard_map(
        local,
        mesh=torus,
        in_specs=(
            P(DP, MP, None, None, None),
            P(MP, None, DP, None),
            P(None, MP, None, DP, None),
            P(None, MP, None, DP, None),
            P(),
            P(),
            P(),
            P(),
            P(),
        ),
        out_specs=(
            P(MP, None, None, None),
            P(MP, None, DP, None),
            P(None, MP, None, DP, None),
            P(None, MP, None, DP, None),
            P(MP, None, DP, None),
        ),
        check_vma=False,
    )
```

```python
import jax
import jax.numpy as jnp
from jax import lax
from jax.experimental import pallas as pl
from jax.experimental.pallas import tpu as pltpu
from jax.sharding import Mesh
from jax.sharding import PartitionSpec as P

D = 4608
HQ = 4096
DP = ("hi", "lo")
MP = ("mp_0", "mp_1", "mp_2")
PLANE = ("mp_0", "mp_1")
COLUMN = ("hi", "lo", "mp_2")
RATES = (0.9, 0.99, 0.999)
FEATS = 8
HIDDEN = 4
NT = 2
LANES = 128
STEP = 32
TAIL = 16
GRADES = 8

VMEM = pl.BlockSpec(memory_space=pltpu.VMEM)
SMEM = pl.BlockSpec(memory_space=pltpu.SMEM)
HBM = pl.BlockSpec(memory_space=pltpu.HBM)
PARAMS = pltpu.CompilerParams(vmem_limit_bytes=6 << 20)


def reduced_gradient(parts):
    hi_count, lo_count = lax.axis_size("hi"), lax.axis_size("lo")
    count = hi_count * lo_count
    lo = lax.axis_index("lo")
    nt, rows, lanes = parts.shape
    blocks = parts.reshape(nt, hi_count, lo_count, rows // count, lanes)

    def of_class(shift):
        return lax.dynamic_index_in_dim(blocks, (lo + shift) % lo_count, 2, keepdims=False)

    from_below = lax.ppermute(of_class(1), DP, [(i, (i + 1) % count) for i in range(count)])
    from_above = lax.ppermute(of_class(lo_count - 1), DP, [(i, (i - 1) % count) for i in range(count)])
    partial = of_class(0).astype(jnp.float32) + from_below.astype(jnp.float32)
    partial = (partial + from_above.astype(jnp.float32)).astype(jnp.bfloat16)
    return lax.all_to_all(jnp.moveaxis(partial, 1, 0), "hi", 0, 0, tiled=True)


def moments_kernel(got, master, momenta, second, features_out, sums_out, table):
    own = master.shape[0] // NT
    table[...] = jnp.zeros_like(table)
    for t in range(NT):

        def body(i, sums):
            rows = pl.ds(pl.multiple_of(t * own + i * STEP, STEP), STEP)
            grad = got[0, rows, :].astype(jnp.float32)
            for k in range(1, got.shape[0]):
                grad = grad + got[k, rows, :].astype(jnp.float32)
            square = grad * grad
            moments, ratios = [], []
            for k, rate in enumerate(RATES):
                moment = rate * momenta[k, rows, :] + (1.0 - rate) * grad
                spread = rate * second[k, rows, :] + (1.0 - rate) * square
                moments.append(moment)
                ratios.append(moment * lax.rsqrt(spread))
            listing = [grad, *moments, *ratios]
            for k, x in enumerate(listing):
                features_out[k, rows, :] = x
            return tuple(
                s + jnp.sum((x * x).reshape(STEP // 8, 8, LANES), axis=0)
                for s, x in zip(sums, [master[rows, :], *listing])
            )

        zeros = tuple(jnp.zeros((8, LANES), jnp.float32) for _ in range(FEATS))
        sums = lax.fori_loop(0, own // STEP, body, zeros)
        for f in range(FEATS):
            k = t * FEATS + f
            table[k : k + 1, :] = jnp.sum(sums[f], axis=0, keepdims=True)
    sums_out[...] = lax.dot_general(
        jnp.ones(sums_out.shape, jnp.float32),
        table[...],
        (((1,), (1,)), ((), ())),
        precision=lax.Precision.HIGHEST,
        preferred_element_type=jnp.float32,
    )


def update_kernel(
    totals, lane_weight, phase, first, bias, last, master, features,
    update_hbm, master_hbm, params_out, scaled, update_out, master_out, done,
):
    rows = master.shape[0]
    own = rows // NT
    total = jnp.sum(totals[...], axis=0, keepdims=True)
    norms = jnp.sqrt(total / float(D * HQ) + 1e-06)
    inverse = 1.0 / norms
    logs = lane_weight[...] * jnp.log(norms)
    lane = lax.broadcasted_iota(jnp.int32, logs.shape, 1)

    def rows_of(x):
        return jnp.broadcast_to(x[None], (STEP // 8, 8, LANES)).reshape(STEP, LANES)

    largest = jnp.zeros((8, LANES), jnp.float32)
    for t in range(NT):
        mine = jnp.where(lane // FEATS == t, logs, 0.0)
        logit = jnp.sum(mine, axis=1, keepdims=True) + phase[0]
        boost = rows_of(jnp.broadcast_to(jnp.exp(jnp.tanh(logit)), (8, LANES)))
        for f in range(FEATS):
            k = t * FEATS + f
            scale = jnp.broadcast_to(inverse[:, k : k + 1], (8, LANES))
            for j in range(HIDDEN):
                scaled[f * HIDDEN + j] = first[f, j] * scale

        def body(i, largest):
            at = pl.ds(pl.multiple_of(t * own + i * STEP, STEP), STEP)
            old = master[at, :]
            listing = [old] + [features[k, at, :] for k in range(FEATS - 1)]
            direction = jnp.zeros((STEP, LANES), jnp.float32)
            magnitude = jnp.zeros((STEP, LANES), jnp.float32)
            for j in range(HIDDEN):
                active = bias[j] + listing[0] * rows_of(scaled[j])
                for f in range(1, FEATS):
                    active = active + listing[f] * rows_of(scaled[f * HIDDEN + j])
                active = jnp.maximum(active, 0.0)
                direction = direction + last[j, 0] * active
                magnitude = magnitude + last[j, 1] * active
            step = direction * jnp.exp(0.5 * jnp.tanh(magnitude)) * boost
            new = old - 0.05 * step
            update_out[at, :] = step
            master_out[at, :] = new
            return jnp.maximum(largest, jnp.max(jnp.abs(new).reshape(STEP // 8, 8, LANES), axis=0))

        largest = lax.fori_loop(0, own // STEP, body, largest)
        half = pl.ds(t * own, own)
        pltpu.make_async_copy(update_out.at[half], update_hbm.at[half], done.at[0, t]).start()
        pltpu.make_async_copy(master_out.at[half], master_hbm.at[half], done.at[1, t]).start()

    most = jnp.max(jnp.max(largest, axis=0, keepdims=True), axis=1, keepdims=True) * 0.125
    power = jnp.full((1, 1), 0.125, jnp.float32)
    grades = jnp.ones((TAIL, LANES), jnp.float32)
    grade = lax.broadcasted_iota(jnp.int32, grades.shape, 0)
    for k in range(GRADES):
        small = most < 8.0
        most = jnp.where(small, most * 4096.0, most)
        power = jnp.where(small, power * 4096.0, power)
        grades = grades * jnp.where(grade == k, jnp.where(small, 1.0 / 4096.0, 1.0), 1.0)
    power = jnp.broadcast_to(power, (STEP, LANES))

    def write(i, carry):
        at = pl.ds(pl.multiple_of(i * STEP, STEP), STEP)
        rounded = master_out[at, :].astype(jnp.bfloat16).astype(jnp.float32)
        params_out[at, :] = (rounded * power).astype(params_out.dtype)
        return carry

    lax.fori_loop(0, rows // STEP, write, 0)
    params_out[rows:, :] = grades.astype(params_out.dtype)
    for t in range(NT):
        half = pl.ds(t * own, own)
        pltpu.make_async_copy(update_out.at[half], update_hbm.at[half], done.at[0, t]).wait()
        pltpu.make_async_copy(master_out.at[half], master_hbm.at[half], done.at[1, t]).wait()


def local(
    grad_parts, master, momenta, second, step_count, mlp_first, mlp_bias, mlp_second, tensor_weight
):
    dp_count = lax.axis_size("hi") * lax.axis_size("lo")
    plane_count = lax.axis_size("mp_0") * lax.axis_size("mp_1")
    column_count = dp_count * lax.axis_size("mp_2")
    _, nt, own, lanes = master.shape
    rows = nt * own
    f32, bf16 = jnp.float32, jnp.bfloat16
    state = jax.ShapeDtypeStruct((rows, lanes), f32)

    got = reduced_gradient(grad_parts[0, 0])
    old_master = master.reshape(rows, lanes)
    old_second = second.reshape(3, rows, lanes)
    features, sums = pl.pallas_call(
        moments_kernel,
        out_shape=(
            jax.ShapeDtypeStruct((FEATS - 1, rows, lanes), f32),
            jax.ShapeDtypeStruct((plane_count, lanes), f32),
        ),
        in_specs=[VMEM] * 4,
        out_specs=(VMEM,) * 2,
        scratch_shapes=[pltpu.VMEM((LANES, LANES), f32)],
        compiler_params=PARAMS,
        name="moments",
    )(got.reshape(-1, rows, lanes), old_master, momenta.reshape(3, rows, lanes), old_second)
    sums = lax.all_to_all(sums, PLANE, 0, 0, tiled=True)
    sums = jnp.broadcast_to(jnp.sum(sums, axis=0), (column_count, lanes))
    sums = lax.all_to_all(sums, COLUMN, 0, 0, tiled=True)

    new_momenta = features[1:4]
    square = features[0] * features[0]
    new_second = jnp.stack(
        [rate * old_second[k] + (1.0 - rate) * square for k, rate in enumerate(RATES)]
    )

    step_value = step_count[0].astype(f32)
    phase = tensor_weight[FEATS] * (jnp.log1p(step_value) / 11.5)
    phase = phase + tensor_weight[FEATS + 1] * (step_value / 100000.0)
    lane_weight = jnp.pad(jnp.tile(tensor_weight[:FEATS], nt), (0, lanes - nt * FEATS))[None]
    update, new_master, params = pl.pallas_call(
        update_kernel,
        out_shape=(state, state, jax.ShapeDtypeStruct((rows + TAIL, lanes), bf16)),
        in_specs=[VMEM, VMEM, SMEM, SMEM, SMEM, SMEM, VMEM, VMEM],
        out_specs=(HBM, HBM, VMEM),
        scratch_shapes=[
            pltpu.VMEM((FEATS * HIDDEN, 8, LANES), f32),
            pltpu.VMEM((rows, lanes), f32),
            pltpu.VMEM((rows, lanes), f32),
            pltpu.SemaphoreType.DMA((2, nt)),
        ],
        compiler_params=PARAMS,
        name="update",
    )(sums, lane_weight, phase[None], mlp_first, mlp_bias, mlp_second, old_master, features)
    params = lax.all_gather(params.astype(jnp.float16), DP, axis=0, tiled=False)
    scale = 8.0 * jnp.prod(params[:, rows : rows + GRADES].astype(f32), axis=1, keepdims=True)
    new_params = jnp.stack(
        [
            (params[:, t * own : (t + 1) * own].astype(f32) * scale).astype(bf16)
            for t in range(nt)
        ]
    ).reshape(1, nt, dp_count * own, lanes)
    shape = master.shape
    return (
        new_params,
        new_master.reshape(shape),
        new_momenta.reshape(3, *shape),
        new_second.reshape(3, *shape),
        update.reshape(shape),
    )


def solution(mesh):
    torus = Mesh(mesh.devices.reshape(mesh.shape["dp"] // 3, 3, 4, 8, 2), (*DP, *MP))
    return jax.shard_map(
        local,
        mesh=torus,
        in_specs=(
            P(DP, MP, None, None, None),
            P(MP, None, DP, None),
            P(None, MP, None, DP, None),
            P(None, MP, None, DP, None),
            P(),
            P(),
            P(),
            P(),
            P(),
        ),
        out_specs=(
            P(MP, None, None, None),
            P(MP, None, DP, None),
            P(None, MP, None, DP, None),
            P(None, MP, None, DP, None),
            P(MP, None, DP, None),
        ),
        check_vma=False,
    )
```

```python
import jax
import jax.numpy as jnp
from jax import lax
from jax.experimental import pallas as pl
from jax.experimental.pallas import tpu as pltpu
from jax.sharding import Mesh
from jax.sharding import PartitionSpec as P

D = 4608
HQ = 4096
DP = ("hi", "lo")
MP = ("mp_0", "mp_1", "mp_2")
PLANE = ("mp_0", "mp_1")
COLUMN = ("hi", "lo", "mp_2")
RATES = (0.9, 0.99, 0.999)
FEATS = 8
HIDDEN = 4
NT = 2
LANES = 128
STEP = 32
TAIL = 16
GRADES = 8
BIAS = FEATS * HIDDEN
LAST = BIAS + HIDDEN
PHASE = LAST + 2 * HIDDEN
LANE_WEIGHT = PHASE + 1

VMEM = pl.BlockSpec(memory_space=pltpu.VMEM)
HBM = pl.BlockSpec(memory_space=pltpu.HBM)
PARAMS = pltpu.CompilerParams(vmem_limit_bytes=6 << 20)


def reduced_gradient(parts):
    hi_count, lo_count = lax.axis_size("hi"), lax.axis_size("lo")
    count = hi_count * lo_count
    lo = lax.axis_index("lo")
    nt, rows, lanes = parts.shape
    blocks = parts.reshape(nt, hi_count, lo_count, rows // count, lanes)

    def of_class(shift):
        return lax.dynamic_index_in_dim(blocks, (lo + shift) % lo_count, 2, keepdims=False)

    from_below = lax.ppermute(of_class(1), DP, [(i, (i + 1) % count) for i in range(count)])
    from_above = lax.ppermute(of_class(lo_count - 1), DP, [(i, (i - 1) % count) for i in range(count)])
    partial = of_class(0).astype(jnp.float32) + from_below.astype(jnp.float32)
    partial = (partial + from_above.astype(jnp.float32)).astype(jnp.bfloat16)
    return lax.all_to_all(jnp.moveaxis(partial, 1, 0), "hi", 0, 0, tiled=True)


def moments_kernel(got, master, momenta, second, features_out, sums_out, table):
    own = master.shape[0] // NT
    table[...] = jnp.zeros_like(table)
    for t in range(NT):

        def body(i, sums):
            rows = pl.ds(pl.multiple_of(t * own + i * STEP, STEP), STEP)
            grad = got[0, rows, :].astype(jnp.float32)
            for k in range(1, got.shape[0]):
                grad = grad + got[k, rows, :].astype(jnp.float32)
            square = grad * grad
            moments, ratios = [], []
            for k, rate in enumerate(RATES):
                moment = rate * momenta[k, rows, :] + (1.0 - rate) * grad
                spread = rate * second[k, rows, :] + (1.0 - rate) * square
                moments.append(moment)
                ratios.append(moment * lax.rsqrt(spread))
            listing = [grad, *moments, *ratios]
            for k, x in enumerate(listing):
                features_out[k, rows, :] = x
            return tuple(
                s + jnp.sum((x * x).reshape(STEP // 8, 8, LANES), axis=0)
                for s, x in zip(sums, [master[rows, :], *listing])
            )

        zeros = tuple(jnp.zeros((8, LANES), jnp.float32) for _ in range(FEATS))
        sums = lax.fori_loop(0, own // STEP, body, zeros)
        for f in range(FEATS):
            k = t * FEATS + f
            table[k : k + 1, :] = jnp.sum(sums[f], axis=0, keepdims=True)
    sums_out[...] = lax.dot_general(
        jnp.ones(sums_out.shape, jnp.float32),
        table[...],
        (((1,), (1,)), ((), ())),
        precision=lax.Precision.HIGHEST,
        preferred_element_type=jnp.float32,
    )


def update_kernel(
    totals, weights, master, features,
    update_hbm, master_hbm, params_out, scaled, update_out, master_out, done,
):
    rows = master.shape[0]
    own = rows // NT
    total = jnp.sum(totals[...], axis=0, keepdims=True)
    norms = jnp.sqrt(total / float(D * HQ) + 1e-06)
    inverse = 1.0 / norms
    logs = weights[LANE_WEIGHT : LANE_WEIGHT + 1, :] * jnp.log(norms)
    lane = lax.broadcasted_iota(jnp.int32, logs.shape, 1)

    def rows_of(x):
        return jnp.broadcast_to(x[None], (STEP // 8, 8, LANES)).reshape(STEP, LANES)

    def constant(k):
        return jnp.broadcast_to(weights[k : k + 1, :], (STEP, LANES))

    largest = jnp.zeros((8, LANES), jnp.float32)
    for t in range(NT):
        mine = jnp.where(lane // FEATS == t, logs, 0.0)
        logit = jnp.sum(mine, axis=1, keepdims=True) + weights[PHASE : PHASE + 1, 0:1]
        boost = rows_of(jnp.broadcast_to(jnp.exp(jnp.tanh(logit)), (8, LANES)))
        for f in range(FEATS):
            k = t * FEATS + f
            scale = jnp.broadcast_to(inverse[:, k : k + 1], (8, LANES))
            for j in range(HIDDEN):
                k = f * HIDDEN + j
                scaled[k] = weights[k : k + 1, :] * scale

        def body(i, largest):
            at = pl.ds(pl.multiple_of(t * own + i * STEP, STEP), STEP)
            old = master[at, :]
            listing = [old] + [features[k, at, :] for k in range(FEATS - 1)]
            direction = jnp.zeros((STEP, LANES), jnp.float32)
            magnitude = jnp.zeros((STEP, LANES), jnp.float32)
            for j in range(HIDDEN):
                active = constant(BIAS + j) + listing[0] * rows_of(scaled[j])
                for f in range(1, FEATS):
                    active = active + listing[f] * rows_of(scaled[f * HIDDEN + j])
                active = jnp.maximum(active, 0.0)
                direction = direction + constant(LAST + 2 * j) * active
                magnitude = magnitude + constant(LAST + 2 * j + 1) * active
            step = direction * jnp.exp(0.5 * jnp.tanh(magnitude)) * boost
            new = old - 0.05 * step
            update_out[at, :] = step
            master_out[at, :] = new
            return jnp.maximum(largest, jnp.max(jnp.abs(new).reshape(STEP // 8, 8, LANES), axis=0))

        largest = lax.fori_loop(0, own // STEP, body, largest)
        half = pl.ds(t * own, own)
        pltpu.make_async_copy(update_out.at[half], update_hbm.at[half], done.at[0, t]).start()
        pltpu.make_async_copy(master_out.at[half], master_hbm.at[half], done.at[1, t]).start()

    most = jnp.max(jnp.max(largest, axis=0, keepdims=True), axis=1, keepdims=True) * 0.125
    power = jnp.full((1, 1), 0.125, jnp.float32)
    grades = jnp.ones((TAIL, LANES), jnp.float32)
    grade = lax.broadcasted_iota(jnp.int32, grades.shape, 0)
    for k in range(GRADES):
        small = most < 8.0
        most = jnp.where(small, most * 4096.0, most)
        power = jnp.where(small, power * 4096.0, power)
        grades = grades * jnp.where(grade == k, jnp.where(small, 1.0 / 4096.0, 1.0), 1.0)
    power = jnp.broadcast_to(power, (STEP, LANES))

    def write(i, carry):
        at = pl.ds(pl.multiple_of(i * STEP, STEP), STEP)
        rounded = master_out[at, :].astype(jnp.bfloat16).astype(jnp.float32)
        params_out[at, :] = (rounded * power).astype(params_out.dtype)
        return carry

    lax.fori_loop(0, rows // STEP, write, 0)
    params_out[rows:, :] = grades.astype(params_out.dtype)
    for t in range(NT):
        half = pl.ds(t * own, own)
        pltpu.make_async_copy(update_out.at[half], update_hbm.at[half], done.at[0, t]).wait()
        pltpu.make_async_copy(master_out.at[half], master_hbm.at[half], done.at[1, t]).wait()


def local(
    grad_parts, master, momenta, second, step_count, mlp_first, mlp_bias, mlp_second, tensor_weight
):
    dp_count = lax.axis_size("hi") * lax.axis_size("lo")
    plane_count = lax.axis_size("mp_0") * lax.axis_size("mp_1")
    column_count = dp_count * lax.axis_size("mp_2")
    _, nt, own, lanes = master.shape
    rows = nt * own
    f32, bf16 = jnp.float32, jnp.bfloat16
    state = jax.ShapeDtypeStruct((rows, lanes), f32)

    got = reduced_gradient(grad_parts[0, 0])
    old_master = master.reshape(rows, lanes)
    old_second = second.reshape(3, rows, lanes)
    features, sums = pl.pallas_call(
        moments_kernel,
        out_shape=(
            jax.ShapeDtypeStruct((FEATS - 1, rows, lanes), f32),
            jax.ShapeDtypeStruct((plane_count, lanes), f32),
        ),
        in_specs=[VMEM] * 4,
        out_specs=(VMEM,) * 2,
        scratch_shapes=[pltpu.VMEM((LANES, LANES), f32)],
        compiler_params=PARAMS,
        name="moments",
    )(got.reshape(-1, rows, lanes), old_master, momenta.reshape(3, rows, lanes), old_second)
    sums = lax.all_to_all(sums, PLANE, 0, 0, tiled=True)
    sums = jnp.broadcast_to(jnp.sum(sums, axis=0), (column_count, lanes))
    sums = lax.all_to_all(sums, COLUMN, 0, 0, tiled=True)

    new_momenta = features[1:4]
    square = features[0] * features[0]
    new_second = jnp.stack(
        [rate * old_second[k] + (1.0 - rate) * square for k, rate in enumerate(RATES)]
    )

    step_value = step_count[0].astype(f32)
    phase = tensor_weight[FEATS] * (jnp.log1p(step_value) / 11.5)
    phase = phase + tensor_weight[FEATS + 1] * (step_value / 100000.0)
    lane_weight = jnp.pad(jnp.tile(tensor_weight[:FEATS], nt), (0, lanes - nt * FEATS))[None]
    flat = jnp.concatenate([mlp_first.reshape(-1), mlp_bias, mlp_second.reshape(-1), phase[None]])
    weights = jnp.concatenate([jnp.broadcast_to(flat[:, None], (flat.shape[0], lanes)), lane_weight])
    update, new_master, params = pl.pallas_call(
        update_kernel,
        out_shape=(state, state, jax.ShapeDtypeStruct((rows + TAIL, lanes), bf16)),
        in_specs=[VMEM] * 4,
        out_specs=(HBM, HBM, VMEM),
        scratch_shapes=[
            pltpu.VMEM((FEATS * HIDDEN, 8, LANES), f32),
            pltpu.VMEM((rows, lanes), f32),
            pltpu.VMEM((rows, lanes), f32),
            pltpu.SemaphoreType.DMA((2, nt)),
        ],
        compiler_params=PARAMS,
        name="update",
    )(sums, weights, old_master, features)
    params = lax.all_gather(params.astype(jnp.float16), DP, axis=0, tiled=False)
    scale = 8.0 * jnp.prod(params[:, rows : rows + GRADES].astype(f32), axis=1, keepdims=True)
    new_params = jnp.stack(
        [
            (params[:, t * own : (t + 1) * own].astype(f32) * scale).astype(bf16)
            for t in range(nt)
        ]
    ).reshape(1, nt, dp_count * own, lanes)
    shape = master.shape
    return (
        new_params,
        new_master.reshape(shape),
        new_momenta.reshape(3, *shape),
        new_second.reshape(3, *shape),
        update.reshape(shape),
    )


def solution(mesh):
    torus = Mesh(mesh.devices.reshape(mesh.shape["dp"] // 3, 3, 4, 8, 2), (*DP, *MP))
    return jax.shard_map(
        local,
        mesh=torus,
        in_specs=(
            P(DP, MP, None, None, None),
            P(MP, None, DP, None),
            P(None, MP, None, DP, None),
            P(None, MP, None, DP, None),
            P(),
            P(),
            P(),
            P(),
            P(),
        ),
        out_specs=(
            P(MP, None, None, None),
            P(MP, None, DP, None),
            P(None, MP, None, DP, None),
            P(None, MP, None, DP, None),
            P(MP, None, DP, None),
        ),
        check_vma=False,
    )
```

```python
import jax
import jax.numpy as jnp
from jax import lax
from jax.experimental import pallas as pl
from jax.experimental.pallas import tpu as pltpu
from jax.sharding import Mesh
from jax.sharding import PartitionSpec as P

D = 4608
HQ = 4096
DP = ("hi", "lo")
MP = ("mp_0", "mp_1", "mp_2")
PLANE = ("mp_0", "mp_1")
COLUMN = ("hi", "lo", "mp_2")
RATES = (0.9, 0.99, 0.999)
FEATS = 8
HIDDEN = 4
NT = 2
LANES = 128
STEP = 32
TAIL = 8
GRADES = 8
BIAS = FEATS * HIDDEN
LAST = BIAS + HIDDEN
PHASE = LAST + 2 * HIDDEN
LANE_WEIGHT = PHASE + 1

VMEM = pl.BlockSpec(memory_space=pltpu.VMEM)
HBM = pl.BlockSpec(memory_space=pltpu.HBM)
PARAMS = pltpu.CompilerParams(vmem_limit_bytes=6 << 20)


def reduced_gradient(parts):
    hi_count, lo_count = lax.axis_size("hi"), lax.axis_size("lo")
    count = hi_count * lo_count
    lo = lax.axis_index("lo")
    nt, rows, lanes = parts.shape
    blocks = parts.reshape(nt, hi_count, lo_count, rows // count, lanes)

    def of_class(shift):
        return lax.dynamic_index_in_dim(blocks, (lo + shift) % lo_count, 2, keepdims=False)

    from_below = lax.ppermute(of_class(1), DP, [(i, (i + 1) % count) for i in range(count)])
    from_above = lax.ppermute(of_class(lo_count - 1), DP, [(i, (i - 1) % count) for i in range(count)])
    partial = of_class(0).astype(jnp.float32) + from_below.astype(jnp.float32)
    partial = (partial + from_above.astype(jnp.float32)).astype(jnp.bfloat16)
    return lax.all_to_all(jnp.moveaxis(partial, 1, 0), "hi", 0, 0, tiled=True)


def moments_kernel(got, master, momenta, second, features_out, sums_out, table):
    own = master.shape[0] // NT
    table[...] = jnp.zeros_like(table)
    for t in range(NT):

        def body(i, sums):
            rows = pl.ds(pl.multiple_of(t * own + i * STEP, STEP), STEP)
            grad = got[0, rows, :].astype(jnp.float32)
            for k in range(1, got.shape[0]):
                grad = grad + got[k, rows, :].astype(jnp.float32)
            square = grad * grad
            moments, ratios = [], []
            for k, rate in enumerate(RATES):
                moment = rate * momenta[k, rows, :] + (1.0 - rate) * grad
                spread = rate * second[k, rows, :] + (1.0 - rate) * square
                moments.append(moment)
                ratios.append(moment * lax.rsqrt(spread))
            listing = [grad, *moments, *ratios]
            for k, x in enumerate(listing):
                features_out[k, rows, :] = x
            return tuple(
                s + jnp.sum((x * x).reshape(STEP // 8, 8, LANES), axis=0)
                for s, x in zip(sums, [master[rows, :], *listing])
            )

        zeros = tuple(jnp.zeros((8, LANES), jnp.float32) for _ in range(FEATS))
        sums = lax.fori_loop(0, own // STEP, body, zeros)
        for f in range(FEATS):
            k = t * FEATS + f
            table[k : k + 1, :] = jnp.sum(sums[f], axis=0, keepdims=True)
    sums_out[...] = lax.dot_general(
        jnp.ones(sums_out.shape, jnp.float32),
        table[...],
        (((1,), (1,)), ((), ())),
        precision=lax.Precision.HIGHEST,
        preferred_element_type=jnp.float32,
    )


def update_kernel(
    totals, weights, master, features,
    update_hbm, master_hbm, params_out, scaled, update_out, master_out, done,
):
    rows = master.shape[0]
    own = rows // NT
    total = jnp.sum(totals[...], axis=0, keepdims=True)
    norms = jnp.sqrt(total / float(D * HQ) + 1e-06)
    inverse = 1.0 / norms
    logs = weights[LANE_WEIGHT : LANE_WEIGHT + 1, :] * jnp.log(norms)
    lane = lax.broadcasted_iota(jnp.int32, logs.shape, 1)

    def rows_of(x):
        return jnp.broadcast_to(x[None], (STEP // 8, 8, LANES)).reshape(STEP, LANES)

    def constant(k):
        return jnp.broadcast_to(weights[k : k + 1, :], (STEP, LANES))

    largest = jnp.zeros((8, LANES), jnp.float32)
    for t in range(NT):
        mine = jnp.where(lane // FEATS == t, logs, 0.0)
        logit = jnp.sum(mine, axis=1, keepdims=True) + weights[PHASE : PHASE + 1, 0:1]
        boost = rows_of(jnp.broadcast_to(jnp.exp(jnp.tanh(logit)), (8, LANES)))
        for f in range(FEATS):
            k = t * FEATS + f
            scale = jnp.broadcast_to(inverse[:, k : k + 1], (8, LANES))
            for j in range(HIDDEN):
                k = f * HIDDEN + j
                scaled[k] = weights[k : k + 1, :] * scale

        def body(i, largest):
            at = pl.ds(pl.multiple_of(t * own + i * STEP, STEP), STEP)
            old = master[at, :]
            listing = [old] + [features[k, at, :] for k in range(FEATS - 1)]
            direction = jnp.zeros((STEP, LANES), jnp.float32)
            magnitude = jnp.zeros((STEP, LANES), jnp.float32)
            for j in range(HIDDEN):
                active = constant(BIAS + j) + listing[0] * rows_of(scaled[j])
                for f in range(1, FEATS):
                    active = active + listing[f] * rows_of(scaled[f * HIDDEN + j])
                active = jnp.maximum(active, 0.0)
                direction = direction + constant(LAST + 2 * j) * active
                magnitude = magnitude + constant(LAST + 2 * j + 1) * active
            step = direction * jnp.exp(0.5 * jnp.tanh(magnitude)) * boost
            new = old - 0.05 * step
            update_out[at, :] = step
            master_out[at, :] = new
            return jnp.maximum(largest, jnp.max(jnp.abs(new).reshape(STEP // 8, 8, LANES), axis=0))

        largest = lax.fori_loop(0, own // STEP, body, largest)
        half = pl.ds(t * own, own)
        pltpu.make_async_copy(update_out.at[half], update_hbm.at[half], done.at[0, t]).start()
        pltpu.make_async_copy(master_out.at[half], master_hbm.at[half], done.at[1, t]).start()

    most = jnp.max(jnp.max(largest, axis=0, keepdims=True), axis=1, keepdims=True) * 0.125
    power = jnp.full((1, 1), 0.125, jnp.float32)
    grades = jnp.ones((TAIL, LANES), jnp.float32)
    grade = lax.broadcasted_iota(jnp.int32, grades.shape, 0)
    for k in range(GRADES):
        small = most < 8.0
        most = jnp.where(small, most * 4096.0, most)
        power = jnp.where(small, power * 4096.0, power)
        grades = grades * jnp.where(grade == k, jnp.where(small, 1.0 / 4096.0, 1.0), 1.0)
    power = jnp.broadcast_to(power, (STEP, LANES))

    def write(i, carry):
        at = pl.ds(pl.multiple_of(i * STEP, STEP), STEP)
        rounded = master_out[at, :].astype(jnp.bfloat16).astype(jnp.float32)
        params_out[at, :] = (rounded * power).astype(params_out.dtype)
        return carry

    lax.fori_loop(0, rows // STEP, write, 0)
    params_out[rows:, :] = grades.astype(params_out.dtype)
    for t in range(NT):
        half = pl.ds(t * own, own)
        pltpu.make_async_copy(update_out.at[half], update_hbm.at[half], done.at[0, t]).wait()
        pltpu.make_async_copy(master_out.at[half], master_hbm.at[half], done.at[1, t]).wait()


def local(
    grad_parts, master, momenta, second, step_count, mlp_first, mlp_bias, mlp_second, tensor_weight
):
    dp_count = lax.axis_size("hi") * lax.axis_size("lo")
    plane_count = lax.axis_size("mp_0") * lax.axis_size("mp_1")
    column_count = dp_count * lax.axis_size("mp_2")
    _, nt, own, lanes = master.shape
    rows = nt * own
    f32, bf16 = jnp.float32, jnp.bfloat16
    state = jax.ShapeDtypeStruct((rows, lanes), f32)

    got = reduced_gradient(grad_parts[0, 0])
    old_master = master.reshape(rows, lanes)
    old_second = second.reshape(3, rows, lanes)
    features, sums = pl.pallas_call(
        moments_kernel,
        out_shape=(
            jax.ShapeDtypeStruct((FEATS - 1, rows, lanes), f32),
            jax.ShapeDtypeStruct((plane_count, lanes), f32),
        ),
        in_specs=[VMEM] * 4,
        out_specs=(VMEM,) * 2,
        scratch_shapes=[pltpu.VMEM((LANES, LANES), f32)],
        compiler_params=PARAMS,
        name="moments",
    )(got.reshape(-1, rows, lanes), old_master, momenta.reshape(3, rows, lanes), old_second)
    sums = lax.all_to_all(sums, PLANE, 0, 0, tiled=True)
    sums = jnp.broadcast_to(jnp.sum(sums, axis=0), (column_count, lanes))
    sums = lax.all_to_all(sums, COLUMN, 0, 0, tiled=True)

    new_momenta = features[1:4]
    square = features[0] * features[0]
    new_second = jnp.stack(
        [rate * old_second[k] + (1.0 - rate) * square for k, rate in enumerate(RATES)]
    )

    step_value = step_count[0].astype(f32)
    phase = tensor_weight[FEATS] * (jnp.log1p(step_value) / 11.5)
    phase = phase + tensor_weight[FEATS + 1] * (step_value / 100000.0)
    lane_weight = jnp.pad(jnp.tile(tensor_weight[:FEATS], nt), (0, lanes - nt * FEATS))[None]
    flat = jnp.concatenate([mlp_first.reshape(-1), mlp_bias, mlp_second.reshape(-1), phase[None]])
    weights = jnp.concatenate([jnp.broadcast_to(flat[:, None], (flat.shape[0], lanes)), lane_weight])
    update, new_master, params = pl.pallas_call(
        update_kernel,
        out_shape=(state, state, jax.ShapeDtypeStruct((rows + TAIL, lanes), bf16)),
        in_specs=[VMEM] * 4,
        out_specs=(HBM, HBM, VMEM),
        scratch_shapes=[
            pltpu.VMEM((FEATS * HIDDEN, 8, LANES), f32),
            pltpu.VMEM((rows, lanes), f32),
            pltpu.VMEM((rows, lanes), f32),
            pltpu.SemaphoreType.DMA((2, nt)),
        ],
        compiler_params=PARAMS,
        name="update",
    )(sums, weights, old_master, features)
    params = lax.all_gather(params.astype(jnp.float16), DP, axis=0, tiled=False)
    scale = 8.0 * jnp.prod(params[:, rows : rows + GRADES].astype(f32), axis=1, keepdims=True)
    new_params = jnp.stack(
        [
            (params[:, t * own : (t + 1) * own].astype(f32) * scale).astype(bf16)
            for t in range(nt)
        ]
    ).reshape(1, nt, dp_count * own, lanes)
    shape = master.shape
    return (
        new_params,
        new_master.reshape(shape),
        new_momenta.reshape(3, *shape),
        new_second.reshape(3, *shape),
        update.reshape(shape),
    )


def solution(mesh):
    torus = Mesh(mesh.devices.reshape(mesh.shape["dp"] // 3, 3, 4, 8, 2), (*DP, *MP))
    return jax.shard_map(
        local,
        mesh=torus,
        in_specs=(
            P(DP, MP, None, None, None),
            P(MP, None, DP, None),
            P(None, MP, None, DP, None),
            P(None, MP, None, DP, None),
            P(),
            P(),
            P(),
            P(),
            P(),
        ),
        out_specs=(
            P(MP, None, None, None),
            P(MP, None, DP, None),
            P(None, MP, None, DP, None),
            P(None, MP, None, DP, None),
            P(MP, None, DP, None),
        ),
        check_vma=False,
    )
```

```python
import jax
import jax.numpy as jnp
from jax import lax
from jax.experimental import pallas as pl
from jax.experimental.pallas import tpu as pltpu
from jax.sharding import Mesh
from jax.sharding import PartitionSpec as P

D = 4608
HQ = 4096
DP = ("hi", "lo")
MP = ("mp_0", "mp_1", "mp_2")
PLANE = ("mp_0", "mp_1")
COLUMN = ("hi", "lo", "mp_2")
RATES = (0.9, 0.99, 0.999)
FEATS = 8
HIDDEN = 4
NT = 2
LANES = 128
STEP = 32
TAIL = 8
GRADES = 8
BIAS = FEATS * HIDDEN
LAST = BIAS + HIDDEN
PHASE = LAST + 2 * HIDDEN
LANE_WEIGHT = PHASE + 1

VMEM = pl.BlockSpec(memory_space=pltpu.VMEM)
HBM = pl.BlockSpec(memory_space=pltpu.HBM)
PARAMS = pltpu.CompilerParams(vmem_limit_bytes=6 << 20)


def reduced_gradient(parts):
    hi_count, lo_count = lax.axis_size("hi"), lax.axis_size("lo")
    count = hi_count * lo_count
    lo = lax.axis_index("lo")
    nt, rows, lanes = parts.shape
    blocks = parts.reshape(nt, hi_count, lo_count, rows // count, lanes)

    def of_class(shift):
        return lax.dynamic_index_in_dim(blocks, (lo + shift) % lo_count, 2, keepdims=False)

    from_below = lax.ppermute(of_class(1), DP, [(i, (i + 1) % count) for i in range(count)])
    from_above = lax.ppermute(of_class(lo_count - 1), DP, [(i, (i - 1) % count) for i in range(count)])
    partial = of_class(0).astype(jnp.float32) + from_below.astype(jnp.float32)
    partial = (partial + from_above.astype(jnp.float32)).astype(jnp.bfloat16)
    return lax.all_to_all(jnp.moveaxis(partial, 1, 0), "hi", 0, 0, tiled=True)


def moments_kernel(got, master, momenta, second, features_out, sums_out, table):
    own = master.shape[0] // NT
    table[...] = jnp.zeros_like(table)
    for t in range(NT):

        def body(i, sums):
            rows = pl.ds(pl.multiple_of(t * own + i * STEP, STEP), STEP)
            grad = got[0, rows, :].astype(jnp.float32)
            for k in range(1, got.shape[0]):
                grad = grad + got[k, rows, :].astype(jnp.float32)
            square = grad * grad
            moments, ratios = [], []
            for k, rate in enumerate(RATES):
                moment = rate * momenta[k, rows, :] + (1.0 - rate) * grad
                spread = rate * second[k, rows, :] + (1.0 - rate) * square
                moments.append(moment)
                ratios.append(moment * lax.rsqrt(spread))
            listing = [grad, *moments, *ratios]
            for k, x in enumerate(listing):
                features_out[k, rows, :] = x
            return tuple(
                s + jnp.sum((x * x).reshape(STEP // 8, 8, LANES), axis=0)
                for s, x in zip(sums, [master[rows, :], *listing])
            )

        zeros = tuple(jnp.zeros((8, LANES), jnp.float32) for _ in range(FEATS))
        sums = lax.fori_loop(0, own // STEP, body, zeros)
        for f in range(FEATS):
            k = t * FEATS + f
            table[k : k + 1, :] = jnp.sum(sums[f], axis=0, keepdims=True)
    ones = jnp.ones((sums_out.shape[0], LANES), jnp.bfloat16)
    left = table[...]
    sums = jnp.zeros(sums_out.shape, jnp.float32)
    for _ in range(3):
        part = left.astype(jnp.bfloat16)
        left = left - part.astype(jnp.float32)
        sums = sums + lax.dot_general(
            ones, part, (((1,), (1,)), ((), ())), preferred_element_type=jnp.float32
        )
    sums_out[...] = sums


def update_kernel(
    totals, weights, master, features,
    update_hbm, master_hbm, params_out, scaled, update_out, master_out, done,
):
    rows = master.shape[0]
    own = rows // NT
    total = jnp.sum(totals[...], axis=0, keepdims=True)
    norms = jnp.sqrt(total / float(D * HQ) + 1e-06)
    inverse = 1.0 / norms
    logs = weights[LANE_WEIGHT : LANE_WEIGHT + 1, :] * jnp.log(norms)
    lane = lax.broadcasted_iota(jnp.int32, logs.shape, 1)

    def rows_of(x):
        return jnp.broadcast_to(x[None], (STEP // 8, 8, LANES)).reshape(STEP, LANES)

    def constant(k):
        return jnp.broadcast_to(weights[k : k + 1, :], (STEP, LANES))

    largest = jnp.zeros((8, LANES), jnp.float32)
    for t in range(NT):
        mine = jnp.where(lane // FEATS == t, logs, 0.0)
        logit = jnp.sum(mine, axis=1, keepdims=True) + weights[PHASE : PHASE + 1, 0:1]
        boost = rows_of(jnp.broadcast_to(jnp.exp(jnp.tanh(logit)), (8, LANES)))
        for f in range(FEATS):
            k = t * FEATS + f
            scale = jnp.broadcast_to(inverse[:, k : k + 1], (8, LANES))
            for j in range(HIDDEN):
                k = f * HIDDEN + j
                scaled[k] = weights[k : k + 1, :] * scale

        def body(i, largest):
            at = pl.ds(pl.multiple_of(t * own + i * STEP, STEP), STEP)
            old = master[at, :]
            listing = [old] + [features[k, at, :] for k in range(FEATS - 1)]
            direction = jnp.zeros((STEP, LANES), jnp.float32)
            magnitude = jnp.zeros((STEP, LANES), jnp.float32)
            for j in range(HIDDEN):
                active = constant(BIAS + j) + listing[0] * rows_of(scaled[j])
                for f in range(1, FEATS):
                    active = active + listing[f] * rows_of(scaled[f * HIDDEN + j])
                active = jnp.maximum(active, 0.0)
                direction = direction + constant(LAST + 2 * j) * active
                magnitude = magnitude + constant(LAST + 2 * j + 1) * active
            step = direction * jnp.exp(0.5 * jnp.tanh(magnitude)) * boost
            new = old - 0.05 * step
            update_out[at, :] = step
            master_out[at, :] = new
            return jnp.maximum(largest, jnp.max(jnp.abs(new).reshape(STEP // 8, 8, LANES), axis=0))

        largest = lax.fori_loop(0, own // STEP, body, largest)
        half = pl.ds(t * own, own)
        pltpu.make_async_copy(update_out.at[half], update_hbm.at[half], done.at[0, t]).start()
        pltpu.make_async_copy(master_out.at[half], master_hbm.at[half], done.at[1, t]).start()

    most = jnp.max(jnp.max(largest, axis=0, keepdims=True), axis=1, keepdims=True) * 0.125
    power = jnp.full((1, 1), 0.125, jnp.float32)
    grades = jnp.ones((TAIL, LANES), jnp.float32)
    grade = lax.broadcasted_iota(jnp.int32, grades.shape, 0)
    for k in range(GRADES):
        small = most < 8.0
        most = jnp.where(small, most * 4096.0, most)
        power = jnp.where(small, power * 4096.0, power)
        grades = grades * jnp.where(grade == k, jnp.where(small, 1.0 / 4096.0, 1.0), 1.0)
    power = jnp.broadcast_to(power, (STEP, LANES))

    def write(i, carry):
        at = pl.ds(pl.multiple_of(i * STEP, STEP), STEP)
        rounded = master_out[at, :].astype(jnp.bfloat16).astype(jnp.float32)
        params_out[at, :] = (rounded * power).astype(params_out.dtype)
        return carry

    lax.fori_loop(0, rows // STEP, write, 0)
    params_out[rows:, :] = grades.astype(params_out.dtype)
    for t in range(NT):
        half = pl.ds(t * own, own)
        pltpu.make_async_copy(update_out.at[half], update_hbm.at[half], done.at[0, t]).wait()
        pltpu.make_async_copy(master_out.at[half], master_hbm.at[half], done.at[1, t]).wait()


def local(
    grad_parts, master, momenta, second, step_count, mlp_first, mlp_bias, mlp_second, tensor_weight
):
    dp_count = lax.axis_size("hi") * lax.axis_size("lo")
    plane_count = lax.axis_size("mp_0") * lax.axis_size("mp_1")
    column_count = dp_count * lax.axis_size("mp_2")
    _, nt, own, lanes = master.shape
    rows = nt * own
    f32, bf16 = jnp.float32, jnp.bfloat16
    state = jax.ShapeDtypeStruct((rows, lanes), f32)

    got = reduced_gradient(grad_parts[0, 0])
    old_master = master.reshape(rows, lanes)
    old_second = second.reshape(3, rows, lanes)
    features, sums = pl.pallas_call(
        moments_kernel,
        out_shape=(
            jax.ShapeDtypeStruct((FEATS - 1, rows, lanes), f32),
            jax.ShapeDtypeStruct((plane_count, lanes), f32),
        ),
        in_specs=[VMEM] * 4,
        out_specs=(VMEM,) * 2,
        scratch_shapes=[pltpu.VMEM((LANES, LANES), f32)],
        compiler_params=PARAMS,
        name="moments",
    )(got.reshape(-1, rows, lanes), old_master, momenta.reshape(3, rows, lanes), old_second)
    sums = lax.all_to_all(sums, PLANE, 0, 0, tiled=True)
    sums = jnp.broadcast_to(jnp.sum(sums, axis=0), (column_count, lanes))
    sums = lax.all_to_all(sums, COLUMN, 0, 0, tiled=True)

    new_momenta = features[1:4]
    square = features[0] * features[0]
    new_second = jnp.stack(
        [rate * old_second[k] + (1.0 - rate) * square for k, rate in enumerate(RATES)]
    )

    step_value = step_count[0].astype(f32)
    phase = tensor_weight[FEATS] * (jnp.log1p(step_value) / 11.5)
    phase = phase + tensor_weight[FEATS + 1] * (step_value / 100000.0)
    lane_weight = jnp.pad(jnp.tile(tensor_weight[:FEATS], nt), (0, lanes - nt * FEATS))[None]
    flat = jnp.concatenate([mlp_first.reshape(-1), mlp_bias, mlp_second.reshape(-1), phase[None]])
    weights = jnp.concatenate([jnp.broadcast_to(flat[:, None], (flat.shape[0], lanes)), lane_weight])
    update, new_master, params = pl.pallas_call(
        update_kernel,
        out_shape=(state, state, jax.ShapeDtypeStruct((rows + TAIL, lanes), bf16)),
        in_specs=[VMEM] * 4,
        out_specs=(HBM, HBM, VMEM),
        scratch_shapes=[
            pltpu.VMEM((FEATS * HIDDEN, 8, LANES), f32),
            pltpu.VMEM((rows, lanes), f32),
            pltpu.VMEM((rows, lanes), f32),
            pltpu.SemaphoreType.DMA((2, nt)),
        ],
        compiler_params=PARAMS,
        name="update",
    )(sums, weights, old_master, features)
    params = lax.all_gather(params.astype(jnp.float16), DP, axis=0, tiled=False)
    scale = 8.0 * jnp.prod(params[:, rows : rows + GRADES].astype(f32), axis=1, keepdims=True)
    new_params = jnp.stack(
        [
            (params[:, t * own : (t + 1) * own].astype(f32) * scale).astype(bf16)
            for t in range(nt)
        ]
    ).reshape(1, nt, dp_count * own, lanes)
    shape = master.shape
    return (
        new_params,
        new_master.reshape(shape),
        new_momenta.reshape(3, *shape),
        new_second.reshape(3, *shape),
        update.reshape(shape),
    )


def solution(mesh):
    torus = Mesh(mesh.devices.reshape(mesh.shape["dp"] // 3, 3, 4, 8, 2), (*DP, *MP))
    return jax.shard_map(
        local,
        mesh=torus,
        in_specs=(
            P(DP, MP, None, None, None),
            P(MP, None, DP, None),
            P(None, MP, None, DP, None),
            P(None, MP, None, DP, None),
            P(),
            P(),
            P(),
            P(),
            P(),
        ),
        out_specs=(
            P(MP, None, None, None),
            P(MP, None, DP, None),
            P(None, MP, None, DP, None),
            P(None, MP, None, DP, None),
            P(MP, None, DP, None),
        ),
        check_vma=False,
    )
```
